32 devices in a mesh: lon: 8 (over y, x, core), lat: 4 (over z).
Axes of the slice: x: 2, y: 2, z: 4, core: 2. Of those that a mesh axis runs over, the one named last changes fastest.
Arguments:
- grid_latent: bfloat16 [4, 8, 1024, 512], P('lat', 'lon'), may hold values from -6 to 6
- mesh_latent: bfloat16 [4, 8, 160, 512], P('lat', 'lon'), may hold values from -6 to 6
- edge_geometry: float32 [4, 8, 4, 2048], P('lat', 'lon'), may hold values from -6 to 6
- senders: int32 [4, 8, 2048], P('lat', 'lon'), may hold values from 0 to 1023
- receivers: int32 [4, 8, 2048], P('lat', 'lon'), may hold values from 0 to 1439, as said below
- w_grid: bfloat16 [512, 512], replicated, may hold values from -0.25 to 0.25
- w_mesh: bfloat16 [512, 512], replicated, may hold values from -0.25 to 0.25
- w_edge: float32 [4, 512], replicated, may hold values from -3 to 3
- edge_bias: float32 [512], replicated, may hold values from -3 to 3
- w_message: bfloat16 [512, 512], replicated, may hold values from -0.25 to 0.25
- w_node: bfloat16 [1024, 512], replicated, may hold values from -0.1875 to 0.1875
- w_output: bfloat16 [512, 512], replicated, may hold values from -0.25 to 0.25
- norm_gain: float32 [512], replicated, may hold values from 0.1 to 1.9
- norm_bias: float32 [512], replicated, may hold values from -3 to 3
Outputs:
- mesh_out: bfloat16 [4, 8, 160, 512], P('lat', 'lon')
The draws below stay inside these ranges and needn't reach their ends.
Inputs may be any that keep to these rules, and one draw needn't show every extreme that they name: `receivers`: r // 160 is a neighbour slot s from 0 to 8 (latitude offset s // 3 - 1, longitude offset s % 3 - 1); edges of the first band never name latitude offset -1, those of the last band never +1. For s other than 4, with k = s for s < 4 and k = s - 1 otherwise, the row r % 160 lies in k * 16 to k * 16 + 15 for s = 1, 3, 5, 7 and in k * 16 to k * 16 + 3 for s = 0, 2, 6, 8.
All inputs are finite; a program needn't handle non-finite values.
Results may differ from the reference program's by a relative error of at most 0.0095.
Values may be sent and summed in bfloat16 or wider, within the bound.
A program may use at most 64 MiB of HBM per device.

```python
import jax
import jax.numpy as jnp
from jax import lax

D = 512
M_DEV = 160
B_SIDE = 16
B_CORNER = 4
G_DEV = 1024
E_DEV = 2048
N_LON = 8
N_LAT = 4


def draw_receivers(key, part):
    base = jax.random.fold_in(key, 11)
    key_slot, key_side, key_corner, key_own = jax.random.split(base, 4)
    array_shape = (N_LAT, N_LON, E_DEV)
    raw_slot = jax.random.randint(key_slot, array_shape, 0, 40)
    neighbour = raw_slot - 32
    neighbour = neighbour + (neighbour >= 4).astype(jnp.int32)
    slot_number = jnp.where(raw_slot < 32, 4, neighbour)
    band_index = jnp.arange(N_LAT, dtype=jnp.int32)[:, None, None]
    lat_offset = slot_number // 3
    outside = (band_index == 0) & (lat_offset == 0) | (band_index == N_LAT - 1) & (lat_offset == 2)
    slot_number = jnp.where(outside, 3 + slot_number % 3, slot_number)
    side_row = jax.random.randint(key_side, array_shape, 0, B_SIDE)
    corner_row = jax.random.randint(key_corner, array_shape, 0, B_CORNER)
    own_row = jax.random.randint(key_own, array_shape, 0, M_DEV)
    strip_number = jnp.where(slot_number < 4, slot_number, slot_number - 1)
    is_corner = (slot_number % 2 == 0) & (slot_number != 4)
    border_row = strip_number * B_SIDE + jnp.where(is_corner, corner_row, side_row)
    row_number = jnp.where(slot_number == 4, own_row, border_row)
    return (slot_number * M_DEV + row_number).astype(jnp.int32)


def plant(drawn, own_key, least, high):
    place = [jax.random.randint(jax.random.fold_in(own_key, axis), (), 0, length) for axis, length in enumerate(drawn.shape)]
    main_axis = drawn.shape.index(max(drawn.shape))
    beside = place[:main_axis] + [(place[main_axis] + 1) % drawn.shape[main_axis]] + place[main_axis + 1:]
    return drawn.at[tuple(place)].set(least).at[tuple(beside)].set(high)


def levels(own_key, dims, cuts, least, top_value):
    level = 1.0
    for position, parts in cuts:
        draws = jax.random.uniform(jax.random.fold_in(jax.random.fold_in(own_key, 6), position), (parts,), jnp.float32, least / len(cuts), top_value / len(cuts))
        level = level * jnp.repeat(jnp.exp(draws), dims[position] // parts).reshape((-1,) + (1,) * (len(dims) - 1 - position))
    return level


def scatter_about(rng, extent, spread, bound, cuts=(), kind=jnp.bfloat16):
    level = levels(rng, extent, cuts, -0.22, 0.18) if cuts else 1.0
    result = jax.random.normal(rng, extent, jnp.float32) * spread * level
    return jnp.minimum(jnp.maximum(result, -bound), bound).astype(kind)


def setup_inputs(seed: int = 0) -> dict:
    seeds = jax.random.split(jax.random.key(seed), 15)
    return {
        "grid_latent": scatter_about(seeds[0], (N_LAT, N_LON, G_DEV, D), 1.0, 6.0, ((0, 4), (1, 8))),
        "mesh_latent": scatter_about(seeds[1], (N_LAT, N_LON, M_DEV, D), 1.0, 6.0, ((0, 4), (1, 8))),
        "edge_geometry": scatter_about(seeds[2], (N_LAT, N_LON, 4, E_DEV), 1.0, 6.0, ((0, 4), (1, 8)), jnp.float32),
        "senders": plant(jax.random.randint(seeds[3], (N_LAT, N_LON, E_DEV), 0, G_DEV), jax.random.fold_in(seeds[3], 1), 0, G_DEV - 1).astype(jnp.int32),
        "receivers": draw_receivers(jax.random.fold_in(seeds[14], 71), 0),
        "w_grid": scatter_about(seeds[5], (D, D), D ** -0.5, 0.25),
        "w_mesh": scatter_about(seeds[6], (D, D), D ** -0.5, 0.25),
        "w_edge": scatter_about(seeds[7], (4, D), 4 ** -0.5, 3.0, (), jnp.float32),
        "edge_bias": scatter_about(seeds[8], (D,), 0.5, 3.0, (), jnp.float32),
        "w_message": scatter_about(seeds[9], (D, D), D ** -0.5, 0.25),
        "w_node": scatter_about(seeds[10], (2 * D, D), (2 * D) ** -0.5, 0.1875),
        "w_output": scatter_about(seeds[11], (D, D), D ** -0.5, 0.25),
        "norm_gain": jnp.clip(1.0 + 0.18 * jax.random.normal(seeds[12], (D,), jnp.float32), 0.1, 1.9),
        "norm_bias": scatter_about(seeds[13], (D,), 0.5, 3.0, (), jnp.float32),
    }


def reference(grid_latent, mesh_latent, edge_geometry, senders, receivers, w_grid, w_mesh, w_edge, edge_bias, w_message, w_node, w_output, norm_gain, norm_bias):
    features = mesh_latent.shape[-1]
    mesh_flat = mesh_latent.reshape(-1, features)
    mesh_proj = jnp.dot(mesh_flat, w_mesh, preferred_element_type=jnp.float32)
    lon_index = jnp.arange(N_LON, dtype=jnp.int32)[:, None]

    def one_band(summed, items):
        band_grid, band_senders, band_receivers, band_geometry, band_index = items
        grid_proj = jnp.dot(band_grid.reshape(-1, features), w_grid, preferred_element_type=jnp.float32)
        grid_proj = grid_proj.reshape(N_LON, G_DEV, features)
        gathered = jax.vmap(lambda table, picks: jnp.take(table, picks, axis=0))(grid_proj, band_senders)
        slot_number = band_receivers // M_DEV
        row_number = band_receivers % M_DEV
        target_lat = band_index + slot_number // 3 - 1
        target_lon = (lon_index + slot_number % 3 - 1) % N_LON
        node_ids = ((target_lat * N_LON + target_lon) * M_DEV + row_number).astype(jnp.int32)
        geometry = jnp.einsum('lce,cd->led', band_geometry, w_edge, precision=lax.Precision.HIGHEST)
        preact = gathered + jnp.take(mesh_proj, node_ids, axis=0) + geometry + edge_bias
        hidden = jax.nn.silu(preact).astype(jnp.bfloat16)
        message = jnp.dot(hidden.reshape(-1, features), w_message, preferred_element_type=jnp.float32).astype(jnp.bfloat16)
        summed = summed + jax.ops.segment_sum(message.astype(jnp.float32), node_ids.reshape(-1), num_segments=mesh_flat.shape[0])
        return (summed, None)
    bands = jnp.arange(N_LAT, dtype=jnp.int32)
    start = jnp.zeros(mesh_flat.shape, jnp.float32)
    aggregated, _ = lax.scan(one_band, start, (grid_latent, senders, receivers, edge_geometry, bands))
    node_in = jnp.concatenate([mesh_flat, aggregated.astype(jnp.bfloat16)], axis=1)
    node_hidden = jax.nn.silu(jnp.dot(node_in, w_node, preferred_element_type=jnp.float32)).astype(jnp.bfloat16)
    update = jnp.dot(node_hidden, w_output, preferred_element_type=jnp.float32)
    row_mean = lax.optimization_barrier(jnp.mean(update, axis=-1, keepdims=True))
    centered = update - row_mean
    row_var = lax.optimization_barrier(jnp.mean(centered * centered, axis=-1, keepdims=True))
    normed = centered * lax.rsqrt(row_var + 1e-05) * norm_gain + norm_bias
    mesh_out = (mesh_flat.astype(jnp.float32) + normed).astype(jnp.bfloat16)
    return mesh_out.reshape(mesh_latent.shape)
```

```python
import functools

import jax
import jax.numpy as jnp
from jax import lax
from jax.experimental import pallas as pl
from jax.experimental.pallas import tpu as pltpu
from jax.sharding import PartitionSpec as P

B_SIDE = 16
B_CORNER = 4
TAIL = 16
MESH = pl.DeviceIdType.MESH

BF16 = jnp.bfloat16
F32 = jnp.float32

STRIPS = tuple((s, s if s < 4 else s - 1) for s in range(9) if s != 4)
SIDES = (1, 3, 5, 7)
CORNERS = (0, 2, 6, 8)


def nt(a, b):
    return lax.dot_general(a, b, (((1,), (1,)), ((), ())), preferred_element_type=F32)


def nn(a, b):
    return jnp.dot(a, b, preferred_element_type=F32)


def halves(x):
    high = x.astype(BF16)
    return high, (x - high.astype(F32)).astype(BF16)


def kernel(
    n_lon,
    n_lat,
    grid_h,
    mesh_h,
    geo_h,
    snd_h,
    rcv_h,
    w_grid_h,
    w_mesh_h,
    w_edge_h,
    bias_h,
    w_message_h,
    w_node_h,
    w_output_h,
    gain_h,
    nbias_h,
    out_ref,
    grid_v,
    mesh_v,
    geo_v,
    snd_v,
    rcv_v,
    w_grid_v,
    w_mesh_v,
    w_edge_v,
    bias_v,
    w_message_v,
    w_node_v,
    w_output_v,
    gain_v,
    nbias_v,
    table,
    onehot,
    summed,
    got_mesh,
    put_sum,
    got_sum,
    load_sem,
    send_a,
    recv_a,
    send_b,
    recv_b,
):
    lon = lax.axis_index("lon")
    lat = lax.axis_index("lat")
    rows, features = mesh_v.shape
    grid_rows = grid_v.shape[0]
    edges = snd_v.shape[1]
    side_base = rows
    corner_base = rows + 4 * B_SIDE
    slots = corner_base + 4 * B_CORNER

    sources = [
        (mesh_h.at[0, 0], mesh_v),
        (snd_h.at[0], snd_v),
        (rcv_h.at[0], rcv_v),
        (geo_h.at[0, 0], geo_v),
        (w_edge_h, w_edge_v),
        (bias_h, bias_v),
        (w_grid_h, w_grid_v),
        (grid_h.at[0, 0], grid_v),
        (w_mesh_h, w_mesh_v),
        (w_node_h, w_node_v),
        (w_message_h, w_message_v),
        (w_output_h, w_output_v),
        (gain_h, gain_v),
        (nbias_h, nbias_v),
    ]
    loads = {}
    for number, (source, target) in enumerate(sources):
        copy = pltpu.make_async_copy(source, target, load_sem.at[number])
        copy.start()
        loads[id(target)] = copy

    def loaded(ref):
        loads[id(ref)].wait()

    def there(dlat, dlon):
        return {
            "lat": lat + dlat,
            "lon": lax.rem(lon + dlon + n_lon, n_lon),
        }

    def has(dlat):
        if dlat == 0:
            return None
        return lat > 0 if dlat < 0 else lat < n_lat - 1

    def guarded(dlat, body, other=None):
        condition = has(dlat)
        if condition is None:
            body()
            return
        pl.when(condition)(body)
        if other is not None:
            pl.when(jnp.logical_not(condition))(other)

    barrier = pltpu.get_barrier_semaphore()
    for dlat in (0, -1, 1):

        def greet(dlat=dlat):
            for dlon in (-1, 0, 1):
                if (dlat, dlon) != (0, 0):
                    pl.semaphore_signal(
                        barrier, inc=1, device_id=there(dlat, dlon), device_id_type=MESH
                    )

        guarded(dlat, greet)
    arrivals = 2 + 3 * (lat > 0).astype(jnp.int32) + 3 * (lat < n_lat - 1).astype(jnp.int32)
    pl.semaphore_wait(barrier, arrivals)

    def mesh_copy(slot, k):
        return pltpu.make_async_remote_copy(
            src_ref=mesh_v.at[pl.ds(k * B_SIDE, B_SIDE)],
            dst_ref=got_mesh.at[k],
            send_sem=send_a.at[k],
            recv_sem=recv_a.at[k],
            device_id=there(-(slot // 3 - 1), -(slot % 3 - 1)),
            device_id_type=MESH,
        )

    def sum_copy(slot, k):
        return pltpu.make_async_remote_copy(
            src_ref=put_sum.at[k],
            dst_ref=got_sum.at[k],
            send_sem=send_b.at[k],
            recv_sem=recv_b.at[k],
            device_id=there(slot // 3 - 1, slot % 3 - 1),
            device_id_type=MESH,
        )

    def in_band(dlat):
        return [(s, k) for s, k in STRIPS if s // 3 - 1 == dlat]

    loaded(mesh_v)
    for dlat in (-1, 1, 0):

        def send(dlat=dlat):
            for s, k in in_band(dlat):
                mesh_copy(s, k).start()

        guarded(-dlat, send)

    loaded(snd_v)
    loaded(rcv_v)
    loaded(geo_v)
    picks = rcv_v[...]
    shift, spot = 0, picks
    for s in range(9):
        k = s if s < 4 else s - 1
        if s == 4:
            base = -4 * rows
        elif s in SIDES:
            base = side_base + B_SIDE * SIDES.index(s) - k * B_SIDE - s * rows
        else:
            base = corner_base + B_CORNER * CORNERS.index(s) - k * B_SIDE - s * rows
        if s == 0:
            spot = spot + base
        else:
            spot = spot + jnp.where(picks >= s * rows, base - shift, 0)
        shift = base
    step = min(512, edges)
    for start in range(0, edges, step):
        span = pl.ds(start, step)
        ids = lax.broadcasted_iota(jnp.int32, (grid_rows, step), 0)
        onehot[:grid_rows, span] = jnp.where(ids == snd_v[:, span], 1.0, 0.0).astype(BF16)
        ids = lax.broadcasted_iota(jnp.int32, (slots, step), 0)
        onehot[grid_rows : grid_rows + slots, span] = jnp.where(
            ids == spot[:, start : start + step], 1.0, 0.0
        ).astype(BF16)
    high, low = [part.astype(F32) for part in halves(geo_v[...])]
    ones = jnp.ones((2, edges), F32)
    zeros = jnp.zeros((2, edges), F32)
    onehot[grid_rows + slots :, :] = jnp.concatenate([high, high, low, ones, zeros], 0).astype(BF16)

    loaded(w_grid_v)
    loaded(grid_v)
    w_grid_t = jnp.transpose(w_grid_v[...])
    table[:, :grid_rows] = (0.5 * nt(w_grid_t, grid_v[...])).astype(BF16)

    loaded(w_edge_v)
    loaded(bias_v)
    high, low = [part.astype(F32) for part in halves(w_edge_v[...])]
    bias_high, bias_low = [part.astype(F32) for part in halves(bias_v[...])]
    tail = jnp.concatenate(
        [high, low, high, bias_high, bias_low, jnp.zeros((2, features), F32)], 0
    )
    loaded(w_mesh_v)
    loaded(w_node_v)
    node_own = nn(mesh_v[...], w_node_v[:features, :])

    for dlat in (-1, 0, 1):

        def arrive(dlat=dlat):
            for s, k in in_band(dlat):
                mesh_copy(s, k).wait_recv()

        def nothing(dlat=dlat):
            for s, k in in_band(dlat):
                got_mesh[k] = jnp.zeros(got_mesh.shape[1:], BF16)

        guarded(dlat, arrive, nothing)

    strip = dict(STRIPS)
    corners = jnp.concatenate(
        [got_mesh[strip[s]].astype(F32)[:B_CORNER] for s in CORNERS], 0
    ).astype(BF16)
    mesh_all = jnp.concatenate(
        [mesh_v[...]] + [got_mesh[strip[s]] for s in SIDES] + [corners], 0
    )
    mesh_table = jnp.concatenate([nn(mesh_all, w_mesh_v[...]), tail], 0) * 0.5
    table[:, grid_rows:] = jnp.transpose(mesh_table).astype(BF16)

    for start in range(0, edges, step):
        span = pl.ds(start, step)
        half = nn(table[...], onehot[:, span])
        hidden = (half + half * jnp.tanh(half)).astype(BF16)
        added = nt(onehot[grid_rows:, span], hidden)
        if start == 0:
            summed[...] = added
        else:
            summed[...] += added

    for s in SIDES:
        first = side_base + B_SIDE * SIDES.index(s)
        put_sum[strip[s]] = summed[first : first + B_SIDE, :].astype(BF16)
    for s in CORNERS:
        first = corner_base + B_CORNER * CORNERS.index(s)
        part = summed[first : first + B_CORNER, :]
        rest = jnp.zeros((B_SIDE - B_CORNER, features), F32)
        put_sum[strip[s]] = jnp.concatenate([part, rest], 0).astype(BF16)
    for dlat in (-1, 1, 0):

        def send(dlat=dlat):
            for s, k in in_band(dlat):
                sum_copy(s, k).start()

        guarded(dlat, send)

    loaded(w_message_v)
    loaded(w_output_v)
    loaded(gain_v)
    loaded(nbias_v)
    for dlat in (-1, 0, 1):

        def arrive(dlat=dlat):
            for s, k in in_band(dlat):
                sum_copy(s, k).wait_recv()

        def nothing(dlat=dlat):
            for s, k in in_band(dlat):
                got_sum[k] = jnp.zeros(got_sum.shape[1:], BF16)

        guarded(-dlat, arrive, nothing)

    border = 8 * B_SIDE
    arrived = got_sum[...].astype(F32).reshape(border, features)
    total = summed[:rows, :]
    total = jnp.concatenate([total[:border] + arrived, total[border:]], 0)
    high, low = halves(total)
    gathered = nn(high, w_message_v[...]) + nn(low, w_message_v[...])
    node = node_own + nn(gathered.astype(BF16), w_node_v[features:, :])
    node_hidden = (node * jax.nn.sigmoid(node)).astype(BF16)
    update = nn(node_hidden, w_output_v[...])
    row_mean = jnp.mean(update, axis=-1, keepdims=True)
    centered = update - row_mean
    row_var = jnp.mean(centered * centered, axis=-1, keepdims=True)
    normed = centered * lax.rsqrt(row_var + 1e-05) * gain_v[...] + nbias_v[...]
    out_ref[0, 0] = (mesh_v[...].astype(F32) + normed).astype(BF16)

    for dlat in (-1, 0, 1):

        def sent(dlat=dlat):
            for s, k in in_band(dlat):
                mesh_copy(s, k).wait_send()

        def sent_sum(dlat=dlat):
            for s, k in in_band(dlat):
                sum_copy(s, k).wait_send()

        guarded(-dlat, sent)
        guarded(dlat, sent_sum)


def local(n_lon, n_lat, *args):
    args = [a.reshape(1, -1) if a.ndim == 1 else a for a in args]
    grid_latent, mesh_latent, geometry, senders = args[:4]
    rows, features = mesh_latent.shape[2:]
    grid_rows = grid_latent.shape[2]
    edges = senders.shape[2]
    slots = rows + 4 * B_SIDE + 4 * B_CORNER
    wide = grid_rows + slots + TAIL
    loads = []
    for number, a in enumerate(args):
        shape = a.shape[2:] if number < 3 else a.shape[1:] if number < 5 else a.shape
        loads.append(pltpu.VMEM(shape, a.dtype))
    return pl.pallas_call(
        functools.partial(kernel, n_lon, n_lat),
        out_shape=jax.ShapeDtypeStruct(mesh_latent.shape, BF16),
        in_specs=[pl.BlockSpec(memory_space=pl.ANY)] * len(args),
        out_specs=pl.BlockSpec(memory_space=pltpu.VMEM),
        scratch_shapes=loads
        + [
            pltpu.VMEM((features, wide), BF16),
            pltpu.VMEM((wide, edges), BF16),
            pltpu.VMEM((slots + TAIL, features), F32),
            pltpu.VMEM((8, B_SIDE, features), BF16),
            pltpu.VMEM((8, B_SIDE, features), BF16),
            pltpu.VMEM((8, B_SIDE, features), BF16),
            pltpu.SemaphoreType.DMA((len(args),)),
            pltpu.SemaphoreType.DMA((8,)),
            pltpu.SemaphoreType.DMA((8,)),
            pltpu.SemaphoreType.DMA((8,)),
            pltpu.SemaphoreType.DMA((8,)),
        ],
        compiler_params=pltpu.CompilerParams(
            collective_id=0, has_side_effects=True, vmem_limit_bytes=56 * 1024 * 1024
        ),
    )(*args)


def solution(mesh):
    return jax.shard_map(
        functools.partial(local, mesh.shape["lon"], mesh.shape["lat"]),
        mesh=mesh,
        in_specs=(
            P("lat", "lon", None, None),
            P("lat", "lon", None, None),
            P("lat", "lon", None, None),
            P("lat", "lon", None),
            P("lat", "lon", None),
            P(),
            P(),
            P(),
            P(),
            P(),
            P(),
            P(),
            P(),
            P(),
        ),
        out_specs=P("lat", "lon", None, None),
        check_vma=False,
    )
```

```python
import functools

import jax
import jax.numpy as jnp
from jax import lax
from jax.experimental import pallas as pl
from jax.experimental.pallas import tpu as pltpu
from jax.sharding import PartitionSpec as P

B_SIDE = 16
B_CORNER = 4
TAIL = 16
OFFER_AT = 0
MESH = pl.DeviceIdType.MESH

BF16 = jnp.bfloat16
F32 = jnp.float32

STRIPS = tuple((s, s if s < 4 else s - 1) for s in range(9) if s != 4)
SIDES = (1, 3, 5, 7)
CORNERS = (0, 2, 6, 8)


def nt(a, b):
    return lax.dot_general(a, b, (((1,), (1,)), ((), ())), preferred_element_type=F32)


def nn(a, b):
    return jnp.dot(a, b, preferred_element_type=F32)


def halves(x):
    high = x.astype(BF16)
    return high, (x - high.astype(F32)).astype(BF16)


def kernel(
    n_lon,
    n_lat,
    grid_h,
    mesh_h,
    geo_h,
    snd_h,
    rcv_h,
    w_grid_h,
    w_mesh_h,
    w_edge_h,
    bias_h,
    w_message_h,
    w_node_h,
    w_output_h,
    gain_h,
    nbias_h,
    out_ref,
    grid_v,
    mesh_v,
    geo_v,
    snd_v,
    rcv_v,
    w_grid_v,
    w_mesh_v,
    w_edge_v,
    bias_v,
    w_message_v,
    w_node_v,
    w_output_v,
    gain_v,
    nbias_v,
    table,
    onehot,
    from_grid,
    summed,
    got_mesh,
    put_sum,
    got_sum,
    load_sem,
    send_a,
    recv_a,
    send_b,
    recv_b,
):
    lon = lax.axis_index("lon")
    lat = lax.axis_index("lat")
    rows, features = mesh_v.shape
    grid_rows = grid_v.shape[0]
    edges = snd_v.shape[1]
    side_base = rows
    corner_base = rows + 4 * B_SIDE
    slots = corner_base + 4 * B_CORNER

    sources = [
        (snd_h.at[0], snd_v),
        (w_grid_h, w_grid_v),
        (grid_h.at[0, 0], grid_v),
        (mesh_h.at[0, 0], mesh_v),
        (rcv_h.at[0], rcv_v),
        (geo_h.at[0, 0], geo_v),
        (w_edge_h, w_edge_v),
        (bias_h, bias_v),
        (w_mesh_h, w_mesh_v),
        (w_node_h, w_node_v),
        (w_message_h, w_message_v),
        (w_output_h, w_output_v),
        (gain_h, gain_v),
        (nbias_h, nbias_v),
    ]
    loads = {}
    for number, (source, target) in enumerate(sources):
        copy = pltpu.make_async_copy(source, target, load_sem.at[number])
        copy.start()
        loads[id(target)] = copy

    def loaded(ref):
        loads[id(ref)].wait()

    def there(dlat, dlon):
        return {
            "lat": lat + dlat,
            "lon": lax.rem(lon + dlon + n_lon, n_lon),
        }

    def has(dlat):
        if dlat == 0:
            return None
        return lat > 0 if dlat < 0 else lat < n_lat - 1

    def guarded(dlat, body, other=None):
        condition = has(dlat)
        if condition is None:
            body()
            return
        pl.when(condition)(body)
        if other is not None:
            pl.when(jnp.logical_not(condition))(other)

    barrier = pltpu.get_barrier_semaphore()
    for dlat in (0, -1, 1):

        def greet(dlat=dlat):
            for dlon in (-1, 0, 1):
                if (dlat, dlon) != (0, 0):
                    pl.semaphore_signal(
                        barrier, inc=1, device_id=there(dlat, dlon), device_id_type=MESH
                    )

        guarded(dlat, greet)

    def size_of(slot):
        return B_SIDE if slot in SIDES else B_CORNER

    def mesh_copy(slot, k):
        return pltpu.make_async_remote_copy(
            src_ref=mesh_v.at[pl.ds(k * B_SIDE, size_of(slot))],
            dst_ref=got_mesh.at[k, pl.ds(0, size_of(slot))],
            send_sem=send_a.at[k],
            recv_sem=recv_a.at[k],
            device_id=there(-(slot // 3 - 1), -(slot % 3 - 1)),
            device_id_type=MESH,
        )

    def sum_copy(slot, k):
        return pltpu.make_async_remote_copy(
            src_ref=put_sum.at[k, pl.ds(0, size_of(slot))],
            dst_ref=got_sum.at[k, pl.ds(0, size_of(slot))],
            send_sem=send_b.at[k],
            recv_sem=recv_b.at[k],
            device_id=there(slot // 3 - 1, slot % 3 - 1),
            device_id_type=MESH,
        )

    def in_band(dlat):
        return [(s, k) for s, k in STRIPS if s // 3 - 1 == dlat]

    def offer_strips():
        arrivals = 2 + 3 * (lat > 0).astype(jnp.int32) + 3 * (lat < n_lat - 1).astype(jnp.int32)
        pl.semaphore_wait(barrier, arrivals)
        for dlat in (-1, 1, 0):

            def send(dlat=dlat):
                for s, k in in_band(dlat):
                    mesh_copy(s, k).start()

            guarded(-dlat, send)

    step = min(512, edges)
    starts = list(range(0, edges, step))
    loaded(snd_v)
    for start in starts:
        span = pl.ds(start, step)
        ids = lax.broadcasted_iota(jnp.int32, (grid_rows, step), 0)
        onehot[:grid_rows, span] = jnp.where(ids == snd_v[:, span], 1.0, 0.0).astype(BF16)
    loaded(w_grid_v)
    w_grid_t = jnp.transpose(w_grid_v[...])
    loaded(grid_v)
    table[:, :grid_rows] = (0.5 * nt(w_grid_t, grid_v[...])).astype(BF16)
    loaded(mesh_v)
    for number, start in enumerate(starts):
        if number == OFFER_AT:
            offer_strips()
        span = pl.ds(start, step)
        from_grid[:, span] = nn(table[:, :grid_rows], onehot[:grid_rows, span])
    if OFFER_AT >= len(starts):
        offer_strips()

    loaded(rcv_v)
    loaded(geo_v)
    picks = rcv_v[...]
    shift, spot = 0, picks
    for s in range(9):
        k = s if s < 4 else s - 1
        if s == 4:
            base = -4 * rows
        elif s in SIDES:
            base = side_base + B_SIDE * SIDES.index(s) - k * B_SIDE - s * rows
        else:
            base = corner_base + B_CORNER * CORNERS.index(s) - k * B_SIDE - s * rows
        if s == 0:
            spot = spot + base
        else:
            spot = spot + jnp.where(picks >= s * rows, base - shift, 0)
        shift = base
    for start in starts:
        span = pl.ds(start, step)
        ids = lax.broadcasted_iota(jnp.int32, (slots, step), 0)
        onehot[grid_rows : grid_rows + slots, span] = jnp.where(
            ids == spot[:, start : start + step], 1.0, 0.0
        ).astype(BF16)
    high, low = [part.astype(F32) for part in halves(geo_v[...])]
    ones = jnp.ones((2, edges), F32)
    zeros = jnp.zeros((2, edges), F32)
    onehot[grid_rows + slots :, :] = jnp.concatenate([high, high, low, ones, zeros], 0).astype(BF16)

    loaded(w_edge_v)
    loaded(bias_v)
    high, low = [part.astype(F32) for part in halves(w_edge_v[...])]
    bias_high, bias_low = [part.astype(F32) for part in halves(bias_v[...])]
    tail = jnp.concatenate(
        [high, low, high, bias_high, bias_low, jnp.zeros((2, features), F32)], 0
    )
    loaded(w_mesh_v)
    loaded(w_node_v)
    loaded(w_message_v)
    loaded(w_output_v)
    loaded(gain_v)
    loaded(nbias_v)
    node_own = nn(mesh_v[...], w_node_v[:features, :])

    for dlat in (-1, 0, 1):

        def arrive(dlat=dlat):
            for s, k in in_band(dlat):
                mesh_copy(s, k).wait_recv()

        def nothing(dlat=dlat):
            for s, k in in_band(dlat):
                got_mesh[k] = jnp.zeros(got_mesh.shape[1:], BF16)

        guarded(dlat, arrive, nothing)

    strip = dict(STRIPS)
    corners = jnp.concatenate(
        [got_mesh[strip[s]].astype(F32)[:B_CORNER] for s in CORNERS], 0
    ).astype(BF16)
    mesh_all = jnp.concatenate(
        [mesh_v[...]] + [got_mesh[strip[s]] for s in SIDES] + [corners], 0
    )
    mesh_table = jnp.concatenate([nn(mesh_all, w_mesh_v[...]), tail], 0) * 0.5
    table[:, grid_rows:] = jnp.transpose(mesh_table).astype(BF16)

    for start in range(0, edges, step):
        span = pl.ds(start, step)
        half = from_grid[:, span] + nn(table[:, grid_rows:], onehot[grid_rows:, span])
        hidden = (half + half * jnp.tanh(half)).astype(BF16)
        added = nt(onehot[grid_rows:, span], hidden)
        if start == 0:
            summed[...] = added
        else:
            summed[...] += added

    for s in SIDES:
        first = side_base + B_SIDE * SIDES.index(s)
        put_sum[strip[s]] = summed[first : first + B_SIDE, :].astype(BF16)
    for s in CORNERS:
        first = corner_base + B_CORNER * CORNERS.index(s)
        part = summed[first : first + B_CORNER, :]
        rest = jnp.zeros((B_SIDE - B_CORNER, features), F32)
        put_sum[strip[s]] = jnp.concatenate([part, rest], 0).astype(BF16)
    for dlat in (-1, 1, 0):

        def send(dlat=dlat):
            for s, k in in_band(dlat):
                sum_copy(s, k).start()

        guarded(dlat, send)

    high, low = halves(summed[:rows, :])
    own_message = nn(high, w_message_v[...]) + nn(low, w_message_v[...])
    for dlat in (-1, 0, 1):

        def arrive(dlat=dlat):
            for s, k in in_band(dlat):
                sum_copy(s, k).wait_recv()

        def nothing(dlat=dlat):
            for s, k in in_band(dlat):
                got_sum[k] = jnp.zeros(got_sum.shape[1:], BF16)

        guarded(-dlat, arrive, nothing)

    border = 8 * B_SIDE
    pieces = []
    for s, k in STRIPS:
        piece = got_sum[k]
        if s in CORNERS:
            rest = jnp.zeros((B_SIDE - B_CORNER, features), F32)
            piece = jnp.concatenate([piece.astype(F32)[:B_CORNER], rest], 0).astype(BF16)
        pieces.append(piece)
    border_message = nn(jnp.concatenate(pieces, 0), w_message_v[...])
    gathered = jnp.concatenate(
        [own_message[:border] + border_message, own_message[border:]], 0
    )
    node = node_own + nn(gathered.astype(BF16), w_node_v[features:, :])
    node_hidden = (node * jax.nn.sigmoid(node)).astype(BF16)
    update = nn(node_hidden, w_output_v[...])
    row_mean = jnp.mean(update, axis=-1, keepdims=True)
    centered = update - row_mean
    row_var = jnp.mean(centered * centered, axis=-1, keepdims=True)
    normed = centered * lax.rsqrt(row_var + 1e-05) * gain_v[...] + nbias_v[...]
    out_ref[0, 0] = (mesh_v[...].astype(F32) + normed).astype(BF16)

    for dlat in (-1, 0, 1):

        def sent(dlat=dlat):
            for s, k in in_band(dlat):
                mesh_copy(s, k).wait_send()

        def sent_sum(dlat=dlat):
            for s, k in in_band(dlat):
                sum_copy(s, k).wait_send()

        guarded(-dlat, sent)
        guarded(dlat, sent_sum)


def local(n_lon, n_lat, *args):
    args = [a.reshape(1, -1) if a.ndim == 1 else a for a in args]
    grid_latent, mesh_latent, geometry, senders = args[:4]
    rows, features = mesh_latent.shape[2:]
    grid_rows = grid_latent.shape[2]
    edges = senders.shape[2]
    slots = rows + 4 * B_SIDE + 4 * B_CORNER
    wide = grid_rows + slots + TAIL
    loads = []
    for number, a in enumerate(args):
        shape = a.shape[2:] if number < 3 else a.shape[1:] if number < 5 else a.shape
        loads.append(pltpu.VMEM(shape, a.dtype))
    return pl.pallas_call(
        functools.partial(kernel, n_lon, n_lat),
        out_shape=pltpu.VMEM(mesh_latent.shape, BF16),
        in_specs=[pl.BlockSpec(memory_space=pl.ANY)] * len(args),
        out_specs=pl.BlockSpec(memory_space=pltpu.VMEM),
        scratch_shapes=loads
        + [
            pltpu.VMEM((features, wide), BF16),
            pltpu.VMEM((wide, edges), BF16),
            pltpu.VMEM((features, edges), F32),
            pltpu.VMEM((slots + TAIL, features), F32),
            pltpu.VMEM((8, B_SIDE, features), BF16),
            pltpu.VMEM((8, B_SIDE, features), BF16),
            pltpu.VMEM((8, B_SIDE, features), BF16),
            pltpu.SemaphoreType.DMA((len(args),)),
            pltpu.SemaphoreType.DMA((8,)),
            pltpu.SemaphoreType.DMA((8,)),
            pltpu.SemaphoreType.DMA((8,)),
            pltpu.SemaphoreType.DMA((8,)),
        ],
        compiler_params=pltpu.CompilerParams(
            collective_id=0, has_side_effects=True, vmem_limit_bytes=56 * 1024 * 1024
        ),
    )(*args)


def solution(mesh):
    return jax.shard_map(
        functools.partial(local, mesh.shape["lon"], mesh.shape["lat"]),
        mesh=mesh,
        in_specs=(
            P("lat", "lon", None, None),
            P("lat", "lon", None, None),
            P("lat", "lon", None, None),
            P("lat", "lon", None),
            P("lat", "lon", None),
            P(),
            P(),
            P(),
            P(),
            P(),
            P(),
            P(),
            P(),
            P(),
        ),
        out_specs=P("lat", "lon", None, None),
        check_vma=False,
    )
```
